32 devices in a mesh: band: 32 (over z, y, x, core).
Axes of the slice: x: 2, y: 2, z: 4, core: 2. Of those that a mesh axis runs over, the one named last changes fastest.
Arguments:
- jones_start: float32 [32, 32, 512], P('band'), may hold values from -1.5 to 1.5
- visible: bfloat16 [32, 8, 4096], P('band'), may hold values from -6 to 6
- coherent: bfloat16 [32, 32, 4096], P('band'), may hold values from -1 to 1
- stations: int32 [2, 4096], replicated, may hold values from 0 to 511, as said below
- weights: float32 [32, 512], P('band'), may hold values from 0.2 to 2
- multiplier_start: float32 [32, 32, 512], P('band'), may hold values from -2 to 2
Outputs:
- jones_final: float32 [32, 32, 512], P('band')
- multiplier_final: float32 [32, 32, 512], P('band')
- coefficients: float32 [96, 512], P(None, 'band')
The draws below stay inside these ranges and needn't reach their ends.
Inputs may be any that keep to these rules, and one draw needn't show every extreme that they name: Rows 0 and 1 of each column name two different stations; the same baselines serve every subband.
All inputs are finite; a program needn't handle non-finite values.
Results may differ from the reference program's by a relative error of at most 0.0003.
Values sent between devices are 32-bit elements; how exact they have to be, the bound alone decides.
A program may use at most 64 MiB of HBM per device.

```python
import math
import jax
import jax.numpy as jnp
from jax import lax

N = 512
K = 4
BL = 4096
ITERS = 2
STEPS = 1
BANDS = 32


def draw_stations(key, part):
    first_key = jax.random.fold_in(key, 11)
    second_key = jax.random.fold_in(key, 12)
    leading = jax.random.randint(first_key, (BL,), 0, N, dtype=jnp.int32)
    offset = jax.random.randint(second_key, (BL,), 1, N, dtype=jnp.int32)
    return jnp.stack([leading, (leading + offset) % N]).astype(jnp.int32)


def raised(values, own_key, source, target, blocks, factor):
    def block_of(dim):
        return (jnp.arange(values.shape[dim]) // (values.shape[dim] // blocks)).reshape((-1,) + (1,) * (values.ndim - 1 - dim))

    one_side = jax.random.permutation(own_key, blocks)[block_of(target)]
    far = (block_of(target) + blocks // 2) % blocks
    return jnp.where((block_of(source) == one_side) | (block_of(source) == far), factor * values, values)


def block_levels(own_key, extent, shards, low, high):
    def one(axis_at, shards_of):
        heights = jax.random.uniform(jax.random.fold_in(jax.random.fold_in(own_key, 6), axis_at), (shards_of,), jnp.float32, low / len(shards), high / len(shards))
        return jnp.repeat(jnp.exp(heights), extent[axis_at] // shards_of).reshape((-1,) + (1,) * (len(extent) - axis_at - 1))

    factor_of = one(*shards[0])
    for cut in shards[1:]:
        factor_of = factor_of * one(*cut)
    return factor_of


def centred(rng, extent, width, limit, split=(), held_as=jnp.bfloat16):
    drawn = width * jax.random.normal(rng, extent, jnp.float32)
    if split:
        drawn = drawn * block_levels(rng, extent, split, -0.22, 0.18)
    return jnp.clip(drawn, -limit, limit).astype(held_as)


def heavy_noise(stream_key, extent, scale, limit, pieces, heavy, kind=jnp.bfloat16):
    values = scale * jax.random.normal(stream_key, extent, jnp.float32)
    if pieces:
        values = values * block_levels(stream_key, extent, pieces, -0.22, 0.18)
    return jnp.clip(raised(values, jax.random.fold_in(stream_key, 3), *heavy), -limit, limit).astype(kind)


def setup_inputs(seed: int = 0) -> dict:
    keys = jax.random.split(jax.random.key(seed), 7)
    jones_start = centred(keys[0], (BANDS, 8 * K, N), 0.5, 1.5, ((0, 32),), jnp.float32)
    visible = centred(keys[1], (BANDS, 8, BL), 1.0, 6.0, ((0, 32),))
    coherent = centred(keys[2], (BANDS, 8 * K, BL), 0.3, 1.0, ((0, 32),))
    stations = draw_stations(jax.random.fold_in(keys[6], 71), 0)
    weights = jnp.clip(jnp.exp(math.log(2.0) - 2.3025851 * jax.random.uniform(keys[4], (BANDS, N), jnp.float32) ** block_levels(keys[4], (BANDS, N), ((0, 32),), -0.2, 0.2)), 0.2, 2.0)
    multiplier_start = heavy_noise(keys[5], (BANDS, 8 * K, N), 0.3, 2.0, ((0, 32),), (0, 2, 32, 2.75), jnp.float32)
    return dict(jones_start=jones_start, visible=visible, coherent=coherent, stations=stations, weights=weights, multiplier_start=multiplier_start)


PENALTY = 1.0
STEP_SIZE = 0.05
PAIR_LIST = ((0, 0), (0, 1), (0, 2), (1, 1), (1, 2), (2, 2))

def legendre_basis(band_count):
    position = jnp.arange(band_count, dtype=jnp.float32)
    abscissa = -1.0 + 2.0 * position / (band_count - 1)
    return jnp.stack([jnp.ones_like(abscissa), abscissa, 1.5 * abscissa * abscissa - 0.5])

def matrix_product(first_real, first_imag, second_real, second_imag):

    def contract(lhs_part, rhs_part):
        return lax.optimization_barrier(jnp.sum(lhs_part[:, :, :, None, :] * rhs_part[:, None, :, :, :], axis=2))
    real_part = contract(first_real, second_real) - contract(first_imag, second_imag)
    imag_part = contract(first_real, second_imag) + contract(first_imag, second_real)
    return (real_part, imag_part)

def band_loss(jones_band, visible_band, coherent_band, stations, target_band, multiplier_band, weight_band):
    baseline_count = stations.shape[1]
    direction_count = jones_band.shape[0] // 8
    station_first = jnp.take(jones_band, stations[0], axis=1).reshape(direction_count, 2, 2, 2, baseline_count)
    station_second = jnp.take(jones_band, stations[1], axis=1).reshape(direction_count, 2, 2, 2, baseline_count)
    sky_model = coherent_band.astype(jnp.float32).reshape(direction_count, 2, 2, 2, baseline_count)
    inner_real, inner_imag = matrix_product(station_first[:, 0], station_first[:, 1], sky_model[:, 0], sky_model[:, 1])
    herm_real = jnp.swapaxes(station_second[:, 0], 1, 2)
    herm_imag = -jnp.swapaxes(station_second[:, 1], 1, 2)
    model_real, model_imag = matrix_product(inner_real, inner_imag, herm_real, herm_imag)
    predicted = jnp.stack([lax.optimization_barrier(jnp.sum(model_real, axis=0)), lax.optimization_barrier(jnp.sum(model_imag, axis=0))])
    misfit = visible_band.astype(jnp.float32).reshape(2, 2, 2, baseline_count) - predicted
    data_scale = jones_band.shape[1] / (2.0 * baseline_count)
    distance = jones_band - target_band
    return data_scale * jnp.sum(misfit * misfit) + jnp.sum(multiplier_band * distance) + 0.5 * PENALTY * jnp.sum(weight_band[None, :] * distance * distance)

def descend(jones_band, visible_band, coherent_band, stations, target_band, multiplier_band, weight_band):
    slope_fn = jax.grad(band_loss)
    for inner_turn in range(STEPS):
        slope = slope_fn(jones_band, visible_band, coherent_band, stations, target_band, multiplier_band, weight_band)
        jones_band = jones_band - STEP_SIZE * slope
    return jones_band

def solve_normal(normal_matrix, right_side):
    gram_aa, gram_ab, gram_ac, gram_bb, gram_bc, gram_cc = [normal_matrix[position] for position in range(6)]
    cofac_aa = gram_bb * gram_cc - gram_bc * gram_bc
    cofac_ab = gram_ac * gram_bc - gram_ab * gram_cc
    cofac_ac = gram_ab * gram_bc - gram_ac * gram_bb
    cofac_bb = gram_aa * gram_cc - gram_ac * gram_ac
    cofac_bc = gram_ab * gram_ac - gram_aa * gram_bc
    cofac_cc = gram_aa * gram_bb - gram_ab * gram_ab
    determinant = gram_aa * cofac_aa + gram_ab * cofac_ab + gram_ac * cofac_ac
    inverse_det = 1.0 / determinant
    first_term = right_side[0]
    second_term = right_side[1]
    third_term = right_side[2]
    coeff_a = (cofac_aa * first_term + cofac_ab * second_term + cofac_ac * third_term) * inverse_det
    coeff_b = (cofac_ab * first_term + cofac_bb * second_term + cofac_bc * third_term) * inverse_det
    coeff_c = (cofac_ac * first_term + cofac_bc * second_term + cofac_cc * third_term) * inverse_det
    return jnp.stack([coeff_a, coeff_b, coeff_c])

def reference(jones_start, visible, coherent, stations, weights, multiplier_start):
    band_count = jones_start.shape[0]
    basis_table = legendre_basis(band_count)
    products = jnp.stack([basis_table[first_idx] * basis_table[second_idx] for first_idx, second_idx in PAIR_LIST])
    normal_matrix = PENALTY * jnp.dot(products, weights, precision=lax.Precision.HIGHEST)
    jones_now = jones_start
    multiplier_now = multiplier_start
    coefficients = jnp.zeros((3, jones_start.shape[1], jones_start.shape[2]), jnp.float32)
    for turn_index in range(ITERS):
        combined = multiplier_now + PENALTY * weights[:, None, :] * jones_now
        right_side = jnp.tensordot(basis_table, combined, axes=(1, 0), precision=lax.Precision.HIGHEST)
        coefficients = solve_normal(normal_matrix, right_side)
        target = basis_table[0][:, None, None] * coefficients[0][None] + basis_table[1][:, None, None] * coefficients[1][None] + basis_table[2][:, None, None] * coefficients[2][None]
        multiplier_now = multiplier_now + PENALTY * weights[:, None, :] * (jones_now - target)

        def refine(packed):
            jones_band, visible_band, coherent_band, target_band, multiplier_band, weight_band = packed
            return descend(jones_band, visible_band, coherent_band, stations, target_band, multiplier_band, weight_band)
        jones_now = lax.map(refine, (jones_now, visible, coherent, target, multiplier_now, weights))
    return (jones_now, multiplier_now, coefficients.reshape(coefficients.shape[0] * coefficients.shape[1], coefficients.shape[2]))
```

```python
import functools

import jax
import jax.numpy as jnp
from jax import lax
from jax.experimental import pallas as pl
from jax.experimental.pallas import tpu as pltpu
from jax.sharding import PartitionSpec as P

PENALTY = 1.0
STEP_SIZE = 0.05
MESH = pl.DeviceIdType.MESH
LANES = 128
SUB = 8
GROUP = LANES * SUB


def tile(index):
    return pl.ds(pl.multiple_of(index * SUB, SUB), SUB)


def cmul(a, b):
    return (a[0] * b[0] - a[1] * b[1], a[0] * b[1] + a[1] * b[0])


def cmul_conj(a, b):
    return (a[0] * b[0] + a[1] * b[1], a[1] * b[0] - a[0] * b[1])


def cadd(a, b):
    return (a[0] + b[0], a[1] + b[1])


def basis(f, n):
    x = -1.0 + f.astype(jnp.float32) * (2.0 / (n - 1))
    return x, 1.5 * x * x - 0.5


def kernel(
    n, jones_ref, vis_ref, coh_ref, st_ref, w_ref, mult_ref,
    jout_ref, mout_ref, cout_ref,
    jcur, mcur, cohv, visv, stv, oht, jgat, pbuf, dbuf, xbuf, acc,
    send_a1, recv_a1, send_b1, recv_b1, send_a2, recv_a2, send_b2, recv_b2,
    inv, coefs, ctile, send_sem, recv_sem,
):
    me = lax.axis_index("band")
    rows, stations = jones_ref.shape[1:]
    baselines = vis_ref.shape[2]
    chunks = stations // LANES
    groups = baselines // GROUP
    dirs = rows // 8
    share = stations // n
    scale = stations / (2.0 * baselines)
    all_own = n == rows
    is_owner = me < rows

    def when_owner(fn, otherwise=None):
        if all_own:
            fn()
        else:
            pl.when(is_owner)(fn)
            if otherwise is not None:
                pl.when(jnp.logical_not(is_owner))(otherwise)

    barrier = pltpu.get_barrier_semaphore()

    def greet_all():
        def body(i, _):
            pl.semaphore_signal(barrier, inc=1, device_id=(lax.rem(me + i, n),), device_id_type=MESH)
            return 0
        lax.fori_loop(1, n, body, 0)

    def greet_owners():
        def body(i, _):
            pl.semaphore_signal(barrier, inc=1, device_id=(i,), device_id_type=MESH)
            return 0
        lax.fori_loop(0, rows, body, 0)

    when_owner(greet_all, greet_owners)

    weight = w_ref[...]

    def fill_a(buf, m, j):
        comb = m + PENALTY * weight * j
        for h in range(chunks):
            cut = slice(h * LANES, (h + 1) * LANES)
            buf[pl.ds(h, rows, stride=SUB), :] = comb[:, cut]
            buf[pl.ds(chunks + h, rows, stride=SUB), :] = jnp.broadcast_to(weight[:, cut], (rows, LANES))

    def copy(src, s_idx, dst, d_idx, phase, dest):
        return pltpu.make_async_remote_copy(
            src_ref=src.at[tile(s_idx)], dst_ref=dst.at[tile(d_idx)],
            send_sem=send_sem.at[phase], recv_sem=recv_sem.at[phase],
            device_id=(dest,), device_id_type=MESH)

    def send_a(src, dst, phase):
        def body(i, _):
            c = lax.rem(me + i, rows)

            @pl.when(c != me)
            def _():
                copy(src, c, dst, me, phase, c).start()
            return 0

        if all_own:
            def body(i, _):
                c = lax.rem(me + i, rows)
                copy(src, c, dst, me, phase, c).start()
                return 0
            lax.fori_loop(1, rows, body, 0)
        else:
            lax.fori_loop(0, rows, body, 0)

        def own():
            dst[tile(me), :] = src[tile(me), :]
        when_owner(own)

    def send_b(src, dst, phase):
        def body(i, _):
            d = lax.rem(me + i, n)
            copy(src, d, dst, me, phase, d).start()
            return 0
        lax.fori_loop(1, n, body, 0)
        dst[tile(me), :] = src[tile(me), :]

    def wait_for(ref, slots, sem):
        part = ref.at[pl.ds(0, slots * SUB)]
        pltpu.make_async_copy(part, part, sem).wait()

    fill_a(send_a1, mult_ref[0], jones_ref[0])
    if all_own:
        pl.semaphore_wait(barrier, n - 1)
    else:
        when_owner(lambda: pl.semaphore_wait(barrier, n - 1), lambda: pl.semaphore_wait(barrier, rows))
    send_a(send_a1, recv_a1, 0)
    jcur[...] = jones_ref[0]

    def prep(g, _):
        for s in range(SUB):
            cut = pl.ds(pl.multiple_of(g * GROUP + s * LANES, LANES), LANES)
            cohv[g, pl.ds(s, rows, stride=SUB), :] = coh_ref[0, :, cut].astype(jnp.float32)
            visv[g, pl.ds(s, 8, stride=SUB), :] = vis_ref[0, :, cut].astype(jnp.float32)
            for side in range(2):
                ids = st_ref[side : side + 1, cut]
                stv[g, side * SUB + s : side * SUB + s + 1, :] = ids
                low = jnp.broadcast_to(ids & (LANES - 1), (LANES, LANES))
                hot = low == lax.broadcasted_iota(jnp.int32, (LANES, LANES), 0)
                oht[g, :, side * GROUP + s * LANES : side * GROUP + (s + 1) * LANES] = jnp.where(hot, 1.0, 0.0).astype(jnp.bfloat16)
        return 0

    lax.fori_loop(0, groups, prep, 0)

    def group_step(g, _):
        ids = [stv[g, side * SUB : (side + 1) * SUB, :] for side in range(2)]
        low = [v & (LANES - 1) for v in ids]
        high = [v >> 7 for v in ids]
        pick = [[v == h for h in range(1, chunks)] for v in high]

        def station_value(side, c):
            out = None
            for h in range(chunks):
                row = jnp.broadcast_to(jcur[c : c + 1, h * LANES : (h + 1) * LANES], (SUB, LANES))
                got = jnp.take_along_axis(row, low[side], axis=1)
                out = got if h == 0 else jnp.where(pick[side][h - 1], got, out)
            return out

        def comp(ref, k, i, j):
            base = k * 8 + i * 2 + j
            return (ref(base), ref(base + 4))

        def tiles(ref, offset):
            return lambda c: ref[(offset + c) * SUB : (offset + c + 1) * SUB, :]

        coh = lambda c: cohv[g, c * SUB : (c + 1) * SUB, :]
        vis = lambda c: visv[g, c * SUB : (c + 1) * SUB, :]
        model = [[None, None], [None, None]]
        for k in range(dirs):
            for c in range(k * 8, k * 8 + 8):
                jgat[c * SUB : (c + 1) * SUB, :] = station_value(0, c)
                jgat[(rows + c) * SUB : (rows + c + 1) * SUB, :] = station_value(1, c)
            a = [[comp(tiles(jgat, 0), k, i, j) for j in range(2)] for i in range(2)]
            q = [[comp(tiles(jgat, rows), k, i, j) for j in range(2)] for i in range(2)]
            m = [[comp(coh, k, i, j) for j in range(2)] for i in range(2)]
            for i in range(2):
                inner = [cadd(cmul(a[i][0], m[0][j]), cmul(a[i][1], m[1][j])) for j in range(2)]
                for j in range(2):
                    base = k * 8 + i * 2 + j
                    pbuf[base * SUB : (base + 1) * SUB, :] = inner[j][0]
                    pbuf[(base + 4) * SUB : (base + 5) * SUB, :] = inner[j][1]
                    term = cadd(cmul_conj(inner[0], q[j][0]), cmul_conj(inner[1], q[j][1]))
                    model[i][j] = term if model[i][j] is None else cadd(model[i][j], term)
        resid = [[None, None], [None, None]]
        for i in range(2):
            for j in range(2):
                v = comp(vis, 0, i, j)
                resid[i][j] = tuple((-2.0 * scale) * (v[z] - model[i][j][z]) for z in range(2))
        for k in range(dirs):
            q = [[comp(tiles(jgat, rows), k, i, j) for j in range(2)] for i in range(2)]
            m = [[comp(coh, k, i, j) for j in range(2)] for i in range(2)]
            p = [[comp(tiles(pbuf, 0), k, i, j) for j in range(2)] for i in range(2)]
            for i in range(2):
                x = [cadd(cmul(resid[i][0], q[0][l]), cmul(resid[i][1], q[1][l])) for l in range(2)]
                for j in range(2):
                    ga = cadd(cmul_conj(x[0], m[j][0]), cmul_conj(x[1], m[j][1]))
                    gq = cadd(cmul_conj(p[0][j], resid[0][i]), cmul_conj(p[1][j], resid[1][i]))
                    base = k * 8 + i * 2 + j
                    for z in range(2):
                        c = base + 4 * z
                        dbuf[c * SUB : (c + 1) * SUB, :] = ga[z]
                        dbuf[(rows + c) * SUB : (rows + c + 1) * SUB, :] = gq[z]
        for side in range(2):
            for s in range(SUB):
                d = dbuf[pl.ds(side * rows * SUB + s, rows, stride=SUB), :]
                big = d.astype(jnp.bfloat16)
                small = (d - big.astype(jnp.float32)).astype(jnp.bfloat16)
                which = jnp.broadcast_to(high[side][s : s + 1, :], (rows, LANES))
                at = slice(side * GROUP + s * LANES, side * GROUP + (s + 1) * LANES)
                for h in range(chunks):
                    mask = jnp.where(which == h, 1.0, 0.0).astype(jnp.bfloat16)
                    xbuf[(2 * h) * rows : (2 * h + 1) * rows, at] = big * mask
                    xbuf[(2 * h + 1) * rows : (2 * h + 2) * rows, at] = small * mask
        acc[...] += lax.dot_general(
            xbuf[...], oht[g], (((1,), (1,)), ((), ())), preferred_element_type=jnp.float32)
        return 0

    def data_slope():
        parts = [
            acc[2 * h * rows : (2 * h + 1) * rows, :] + acc[(2 * h + 1) * rows : (2 * h + 2) * rows, :]
            for h in range(chunks)
        ]
        return jnp.concatenate(parts, axis=1)

    row_id = lax.broadcasted_iota(jnp.int32, (SUB, LANES), 0)

    def solve(recv, send, last):
        zero = jnp.zeros((SUB, LANES), jnp.float32)
        if not last:
            def add(f, sums):
                x, y = basis(f, n)
                t = recv[tile(f), :]
                tx, ty = t * x, t * y
                new = (t, tx, ty, tx * x, tx * y, ty * y)
                return tuple(o + v for o, v in zip(sums, new))

            sums = lax.fori_loop(0, n, add, (zero,) * 6, unroll=4)
            aa, ab, ac, bb, bc, cc = [PENALTY * pltpu.roll(v, chunks, 0) for v in sums]
            c_aa = bb * cc - bc * bc
            c_ab = ac * bc - ab * cc
            c_ac = ab * bc - ac * bb
            c_bb = aa * cc - ac * ac
            c_bc = ab * ac - aa * bc
            c_cc = aa * bb - ab * ab
            det = aa * c_aa + ab * c_ab + ac * c_ac
            cof = (c_aa, c_ab, c_ac, c_bb, c_bc, c_cc, 1.0 / det)
            for i, v in enumerate(cof):
                inv[i * SUB : (i + 1) * SUB, :] = v
            right = sums[:3]
        else:
            def add(f, sums):
                x, y = basis(f, n)
                t = recv[tile(f), :]
                return (sums[0] + t, sums[1] + t * x, sums[2] + t * y)

            right = lax.fori_loop(0, n, add, (zero,) * 3, unroll=4)
            cof = [inv[i * SUB : (i + 1) * SUB, :] for i in range(7)]
        c_aa, c_ab, c_ac, c_bb, c_bc, c_cc, inv_det = cof
        r0, r1, r2 = right
        k0 = (c_aa * r0 + c_ab * r1 + c_ac * r2) * inv_det
        k1 = (c_ab * r0 + c_bb * r1 + c_bc * r2) * inv_det
        k2 = (c_ac * r0 + c_bc * r1 + c_cc * r2) * inv_det
        if last:
            ctile[...] = jnp.zeros_like(ctile)
            for p, v in enumerate((k0, k1, k2)):
                coefs[p * SUB : (p + 1) * SUB, :] = v
            for h in range(chunks):
                for p in range(3):
                    ctile[h * SUB + 4 + p : h * SUB + 5 + p, :] = coefs[p * SUB + h : p * SUB + h + 1, :]

        def put(f, _):
            x, y = basis(f, n)
            t = k0 + x * k1 + y * k2
            if last:
                t = jnp.where(row_id < chunks, t, ctile[tile((f * share) // LANES), :])
            send[tile(f), :] = t
            return 0

        lax.fori_loop(0, n, put, 0, unroll=4)

    def owner_turn(recv_a, send_bb, recv_bb, phase, last):
        def go():
            wait_for(recv_a, n - 1, recv_sem.at[phase])
            solve(recv_a, send_bb, last)
            send_b(send_bb, recv_bb, phase + 1)
        when_owner(go)

    def wait_b(recv_bb, phase):
        if all_own:
            wait_for(recv_bb, rows - 1, recv_sem.at[phase])
        else:
            when_owner(lambda: wait_for(recv_bb, rows - 1, recv_sem.at[phase]),
                       lambda: wait_for(recv_bb, rows, recv_sem.at[phase]))

    def target_of(recv_bb):
        return jnp.concatenate([recv_bb[pl.ds(h, rows, stride=SUB), :] for h in range(chunks)], axis=1)

    half = groups // 2

    acc[...] = jnp.zeros_like(acc)
    lax.fori_loop(0, half, group_step, 0)
    owner_turn(recv_a1, send_b1, recv_b1, 0, False)
    lax.fori_loop(half, groups, group_step, 0)
    wait_b(recv_b1, 1)
    jones = jcur[...]
    pull = PENALTY * weight * (jones - target_of(recv_b1))
    mult = mult_ref[0] + pull
    jones = jones - STEP_SIZE * (data_slope() + mult + pull)
    mcur[...] = mult
    jcur[...] = jones
    fill_a(send_a2, mult, jones)
    send_a(send_a2, recv_a2, 2)

    acc[...] = jnp.zeros_like(acc)
    lax.fori_loop(0, half, group_step, 0)
    owner_turn(recv_a2, send_b2, recv_b2, 2, True)
    lax.fori_loop(half, groups, group_step, 0)
    wait_b(recv_b2, 3)
    jones = jcur[...]
    pull = PENALTY * weight * (jones - target_of(recv_b2))
    mult = mcur[...] + pull
    mout_ref[0] = mult
    jout_ref[0] = jones - STEP_SIZE * (data_slope() + mult + pull)
    shift = lax.rem(LANES - lax.rem(me * share, LANES), LANES)
    for p in range(3):
        part = pltpu.roll(recv_b2[pl.ds(4 + p, rows, stride=SUB), :], shift, 1)
        cout_ref[p * rows : (p + 1) * rows, :] = part[:, :share]

    for buf, phase in ((send_a1, 0), (send_a2, 2)):
        if all_own:
            wait_for(buf, rows - 1, send_sem.at[phase])
        else:
            when_owner(functools.partial(wait_for, buf, rows - 1, send_sem.at[phase]),
                       functools.partial(wait_for, buf, rows, send_sem.at[phase]))
    for buf, phase in ((send_b1, 1), (send_b2, 3)):
        when_owner(functools.partial(wait_for, buf, n - 1, send_sem.at[phase]))


def solution(mesh):
    n = mesh.shape["band"]

    def local(jones, visible, coherent, stations, weights, mult):
        rows, count = jones.shape[1:]
        base = visible.shape[2]
        chunks = count // LANES
        groups = base // GROUP
        assert n >= rows and chunks == 4 and LANES % (count // n) == 0
        f32, bf16 = jnp.float32, jnp.bfloat16
        vm = pltpu.VMEM
        flat = lambda slots: vm((slots * SUB, LANES), f32)
        return pl.pallas_call(
            functools.partial(kernel, n),
            out_shape=(
                jax.ShapeDtypeStruct(jones.shape, f32),
                jax.ShapeDtypeStruct(jones.shape, f32),
                jax.ShapeDtypeStruct((3 * rows, count // n), f32),
            ),
            in_specs=[pl.BlockSpec(memory_space=vm)] * 6,
            out_specs=[pl.BlockSpec(memory_space=vm)] * 3,
            scratch_shapes=[
                vm((rows, count), f32),
                vm((rows, count), f32),
                vm((groups, rows * SUB, LANES), f32),
                vm((groups, 8 * SUB, LANES), f32),
                vm((groups, 2 * SUB, LANES), jnp.int32),
                vm((groups, LANES, 2 * GROUP), bf16),
                flat(2 * rows),
                flat(rows),
                flat(2 * rows),
                vm((2 * chunks * rows, 2 * GROUP), bf16),
                vm((2 * chunks * rows, LANES), f32),
                flat(rows), flat(n), flat(n), flat(rows),
                flat(rows), flat(n), flat(n), flat(rows),
                flat(7), flat(3), flat(chunks),
                pltpu.SemaphoreType.DMA((4,)),
                pltpu.SemaphoreType.DMA((4,)),
            ],
            compiler_params=pltpu.CompilerParams(
                collective_id=0, has_side_effects=True, vmem_limit_bytes=40 * 1024 * 1024),
        )(jones, visible, coherent, stations, weights, mult)

    return jax.shard_map(
        local,
        mesh=mesh,
        in_specs=(
            P("band", None, None), P("band", None, None), P("band", None, None),
            P(), P("band", None), P("band", None, None),
        ),
        out_specs=(P("band", None, None), P("band", None, None), P(None, "band")),
        check_vma=False,
    )
```

```python
import functools

import jax
import jax.numpy as jnp
from jax import lax
from jax.experimental import pallas as pl
from jax.experimental.pallas import tpu as pltpu
from jax.sharding import PartitionSpec as P

PENALTY = 1.0
STEP_SIZE = 0.05
MESH = pl.DeviceIdType.MESH
LANES = 128
SUB = 8
GROUP = LANES * SUB


def tile(index):
    return pl.ds(pl.multiple_of(index * SUB, SUB), SUB)


def cmul(a, b):
    return (a[0] * b[0] - a[1] * b[1], a[0] * b[1] + a[1] * b[0])


def cmul_conj(a, b):
    return (a[0] * b[0] + a[1] * b[1], a[1] * b[0] - a[0] * b[1])


def cadd(a, b):
    return (a[0] + b[0], a[1] + b[1])


def basis(f, n):
    x = -1.0 + f.astype(jnp.float32) * (2.0 / (n - 1))
    return x, 1.5 * x * x - 0.5


def kernel(
    n, jones_in, vis_in, coh_in, st_in, w_in, mult_in,
    jout_ref, mout_ref, cout_ref,
    jcur, mcur, cohv, visv, stv, oht, jgat, pbuf, dbuf, xbuf, acc,
    send_a1, recv_a1, send_b1, recv_b1, send_a2, recv_a2, send_b2, recv_b2,
    inv, coefs, ctile, send_sem, recv_sem,
    jones_ref, vis_ref, coh_ref, st_ref, w_ref, mult_ref, load_sem,
):
    loads = [
        pltpu.make_async_copy(src, dst, load_sem.at[i])
        for i, (src, dst) in enumerate((
            (jones_in, jones_ref), (mult_in, mult_ref), (w_in, w_ref),
            (coh_in, coh_ref), (vis_in, vis_ref), (st_in, st_ref)))
    ]
    for load in loads:
        load.start()
    me = lax.axis_index("band")
    rows, stations = jones_ref.shape[1:]
    baselines = vis_ref.shape[2]
    chunks = stations // LANES
    groups = baselines // GROUP
    dirs = rows // 8
    share = stations // n
    scale = stations / (2.0 * baselines)
    all_own = n == rows
    is_owner = me < rows

    def when_owner(fn, otherwise=None):
        if all_own:
            fn()
        else:
            pl.when(is_owner)(fn)
            if otherwise is not None:
                pl.when(jnp.logical_not(is_owner))(otherwise)

    barrier = pltpu.get_barrier_semaphore()

    def greet_all():
        def body(i, _):
            pl.semaphore_signal(barrier, inc=1, device_id=(lax.rem(me + i, n),), device_id_type=MESH)
            return 0
        lax.fori_loop(1, n, body, 0)

    def greet_owners():
        def body(i, _):
            pl.semaphore_signal(barrier, inc=1, device_id=(i,), device_id_type=MESH)
            return 0
        lax.fori_loop(0, rows, body, 0)

    when_owner(greet_all, greet_owners)

    for load in loads[:3]:
        load.wait()
    weight = w_ref[...]

    def fill_a(buf, m, j):
        comb = m + PENALTY * weight * j
        for h in range(chunks):
            cut = slice(h * LANES, (h + 1) * LANES)
            buf[pl.ds(h, rows, stride=SUB), :] = comb[:, cut]
            buf[pl.ds(chunks + h, rows, stride=SUB), :] = jnp.broadcast_to(weight[:, cut], (rows, LANES))

    def copy(src, s_idx, dst, d_idx, phase, dest):
        return pltpu.make_async_remote_copy(
            src_ref=src.at[tile(s_idx)], dst_ref=dst.at[tile(d_idx)],
            send_sem=send_sem.at[phase], recv_sem=recv_sem.at[phase],
            device_id=(dest,), device_id_type=MESH)

    def send_a(src, dst, phase):
        def body(i, _):
            c = lax.rem(me + i, rows)

            @pl.when(c != me)
            def _():
                copy(src, c, dst, me, phase, c).start()
            return 0

        if all_own:
            def body(i, _):
                c = lax.rem(me + i, rows)
                copy(src, c, dst, me, phase, c).start()
                return 0
            lax.fori_loop(1, rows, body, 0)
        else:
            lax.fori_loop(0, rows, body, 0)

        def own():
            dst[tile(me), :] = src[tile(me), :]
        when_owner(own)

    def send_b(src, dst, phase):
        def body(i, _):
            d = lax.rem(me + i, n)
            copy(src, d, dst, me, phase, d).start()
            return 0
        lax.fori_loop(1, n, body, 0)
        dst[tile(me), :] = src[tile(me), :]

    def wait_for(ref, slots, sem):
        part = ref.at[pl.ds(0, slots * SUB)]
        pltpu.make_async_copy(part, part, sem).wait()

    fill_a(send_a1, mult_ref[0], jones_ref[0])
    if all_own:
        pl.semaphore_wait(barrier, n - 1)
    else:
        when_owner(lambda: pl.semaphore_wait(barrier, n - 1), lambda: pl.semaphore_wait(barrier, rows))
    send_a(send_a1, recv_a1, 0)
    jcur[...] = jones_ref[0]
    for load in loads[3:]:
        load.wait()

    def prep(g, _):
        for s in range(SUB):
            cut = pl.ds(pl.multiple_of(g * GROUP + s * LANES, LANES), LANES)
            cohv[g, pl.ds(s, rows, stride=SUB), :] = coh_ref[0, :, cut].astype(jnp.float32)
            visv[g, pl.ds(s, 8, stride=SUB), :] = vis_ref[0, :, cut].astype(jnp.float32)
            for side in range(2):
                ids = st_ref[side : side + 1, cut]
                stv[g, side * SUB + s : side * SUB + s + 1, :] = ids
                low = jnp.broadcast_to(ids & (LANES - 1), (LANES, LANES))
                hot = low == lax.broadcasted_iota(jnp.int32, (LANES, LANES), 0)
                oht[g, :, side * GROUP + s * LANES : side * GROUP + (s + 1) * LANES] = jnp.where(hot, 1.0, 0.0).astype(jnp.bfloat16)
        return 0

    lax.fori_loop(0, groups, prep, 0)

    def group_step(g, _):
        ids = [stv[g, side * SUB : (side + 1) * SUB, :] for side in range(2)]
        low = [v & (LANES - 1) for v in ids]
        high = [v >> 7 for v in ids]
        pick = [[v == h for h in range(1, chunks)] for v in high]

        def station_value(side, c):
            out = None
            for h in range(chunks):
                row = jnp.broadcast_to(jcur[c : c + 1, h * LANES : (h + 1) * LANES], (SUB, LANES))
                got = jnp.take_along_axis(row, low[side], axis=1)
                out = got if h == 0 else jnp.where(pick[side][h - 1], got, out)
            return out

        def comp(ref, k, i, j):
            base = k * 8 + i * 2 + j
            return (ref(base), ref(base + 4))

        def tiles(ref, offset):
            return lambda c: ref[(offset + c) * SUB : (offset + c + 1) * SUB, :]

        coh = lambda c: cohv[g, c * SUB : (c + 1) * SUB, :]
        vis = lambda c: visv[g, c * SUB : (c + 1) * SUB, :]
        model = [[None, None], [None, None]]
        for k in range(dirs):
            for c in range(k * 8, k * 8 + 8):
                jgat[c * SUB : (c + 1) * SUB, :] = station_value(0, c)
                jgat[(rows + c) * SUB : (rows + c + 1) * SUB, :] = station_value(1, c)
            a = [[comp(tiles(jgat, 0), k, i, j) for j in range(2)] for i in range(2)]
            q = [[comp(tiles(jgat, rows), k, i, j) for j in range(2)] for i in range(2)]
            m = [[comp(coh, k, i, j) for j in range(2)] for i in range(2)]
            for i in range(2):
                inner = [cadd(cmul(a[i][0], m[0][j]), cmul(a[i][1], m[1][j])) for j in range(2)]
                for j in range(2):
                    base = k * 8 + i * 2 + j
                    pbuf[base * SUB : (base + 1) * SUB, :] = inner[j][0]
                    pbuf[(base + 4) * SUB : (base + 5) * SUB, :] = inner[j][1]
                    term = cadd(cmul_conj(inner[0], q[j][0]), cmul_conj(inner[1], q[j][1]))
                    model[i][j] = term if model[i][j] is None else cadd(model[i][j], term)
        resid = [[None, None], [None, None]]
        for i in range(2):
            for j in range(2):
                v = comp(vis, 0, i, j)
                resid[i][j] = tuple((-2.0 * scale) * (v[z] - model[i][j][z]) for z in range(2))
        for k in range(dirs):
            q = [[comp(tiles(jgat, rows), k, i, j) for j in range(2)] for i in range(2)]
            m = [[comp(coh, k, i, j) for j in range(2)] for i in range(2)]
            p = [[comp(tiles(pbuf, 0), k, i, j) for j in range(2)] for i in range(2)]
            for i in range(2):
                x = [cadd(cmul(resid[i][0], q[0][l]), cmul(resid[i][1], q[1][l])) for l in range(2)]
                for j in range(2):
                    ga = cadd(cmul_conj(x[0], m[j][0]), cmul_conj(x[1], m[j][1]))
                    gq = cadd(cmul_conj(p[0][j], resid[0][i]), cmul_conj(p[1][j], resid[1][i]))
                    base = k * 8 + i * 2 + j
                    for z in range(2):
                        c = base + 4 * z
                        dbuf[c * SUB : (c + 1) * SUB, :] = ga[z]
                        dbuf[(rows + c) * SUB : (rows + c + 1) * SUB, :] = gq[z]
        for side in range(2):
            for s in range(SUB):
                d = dbuf[pl.ds(side * rows * SUB + s, rows, stride=SUB), :]
                big = d.astype(jnp.bfloat16)
                small = (d - big.astype(jnp.float32)).astype(jnp.bfloat16)
                which = jnp.broadcast_to(high[side][s : s + 1, :], (rows, LANES))
                at = slice(side * GROUP + s * LANES, side * GROUP + (s + 1) * LANES)
                for h in range(chunks):
                    mask = jnp.where(which == h, 1.0, 0.0).astype(jnp.bfloat16)
                    xbuf[(2 * h) * rows : (2 * h + 1) * rows, at] = big * mask
                    xbuf[(2 * h + 1) * rows : (2 * h + 2) * rows, at] = small * mask
        acc[...] += lax.dot_general(
            xbuf[...], oht[g], (((1,), (1,)), ((), ())), preferred_element_type=jnp.float32)
        return 0

    def data_slope():
        parts = [
            acc[2 * h * rows : (2 * h + 1) * rows, :] + acc[(2 * h + 1) * rows : (2 * h + 2) * rows, :]
            for h in range(chunks)
        ]
        return jnp.concatenate(parts, axis=1)

    row_id = lax.broadcasted_iota(jnp.int32, (SUB, LANES), 0)

    def solve(recv, send, last):
        zero = jnp.zeros((SUB, LANES), jnp.float32)
        if not last:
            def add(f, sums):
                x, y = basis(f, n)
                t = recv[tile(f), :]
                tx, ty = t * x, t * y
                new = (t, tx, ty, tx * x, tx * y, ty * y)
                return tuple(o + v for o, v in zip(sums, new))

            sums = lax.fori_loop(0, n, add, (zero,) * 6, unroll=4)
            aa, ab, ac, bb, bc, cc = [PENALTY * pltpu.roll(v, chunks, 0) for v in sums]
            c_aa = bb * cc - bc * bc
            c_ab = ac * bc - ab * cc
            c_ac = ab * bc - ac * bb
            c_bb = aa * cc - ac * ac
            c_bc = ab * ac - aa * bc
            c_cc = aa * bb - ab * ab
            det = aa * c_aa + ab * c_ab + ac * c_ac
            cof = (c_aa, c_ab, c_ac, c_bb, c_bc, c_cc, 1.0 / det)
            for i, v in enumerate(cof):
                inv[i * SUB : (i + 1) * SUB, :] = v
            right = sums[:3]
        else:
            def add(f, sums):
                x, y = basis(f, n)
                t = recv[tile(f), :]
                return (sums[0] + t, sums[1] + t * x, sums[2] + t * y)

            right = lax.fori_loop(0, n, add, (zero,) * 3, unroll=4)
            cof = [inv[i * SUB : (i + 1) * SUB, :] for i in range(7)]
        c_aa, c_ab, c_ac, c_bb, c_bc, c_cc, inv_det = cof
        r0, r1, r2 = right
        k0 = (c_aa * r0 + c_ab * r1 + c_ac * r2) * inv_det
        k1 = (c_ab * r0 + c_bb * r1 + c_bc * r2) * inv_det
        k2 = (c_ac * r0 + c_bc * r1 + c_cc * r2) * inv_det
        if last:
            ctile[...] = jnp.zeros_like(ctile)
            for p, v in enumerate((k0, k1, k2)):
                coefs[p * SUB : (p + 1) * SUB, :] = v
            for h in range(chunks):
                for p in range(3):
                    ctile[h * SUB + 4 + p : h * SUB + 5 + p, :] = coefs[p * SUB + h : p * SUB + h + 1, :]

        def put(f, _):
            x, y = basis(f, n)
            t = k0 + x * k1 + y * k2
            if last:
                t = jnp.where(row_id < chunks, t, ctile[tile((f * share) // LANES), :])
            send[tile(f), :] = t
            return 0

        lax.fori_loop(0, n, put, 0, unroll=4)

    def owner_turn(recv_a, send_bb, recv_bb, phase, last):
        def go():
            wait_for(recv_a, n - 1, recv_sem.at[phase])
            solve(recv_a, send_bb, last)
            send_b(send_bb, recv_bb, phase + 1)
        when_owner(go)

    def wait_b(recv_bb, phase):
        if all_own:
            wait_for(recv_bb, rows - 1, recv_sem.at[phase])
        else:
            when_owner(lambda: wait_for(recv_bb, rows - 1, recv_sem.at[phase]),
                       lambda: wait_for(recv_bb, rows, recv_sem.at[phase]))

    def target_of(recv_bb):
        return jnp.concatenate([recv_bb[pl.ds(h, rows, stride=SUB), :] for h in range(chunks)], axis=1)

    half = groups // 2

    acc[...] = jnp.zeros_like(acc)
    lax.fori_loop(0, half, group_step, 0)
    owner_turn(recv_a1, send_b1, recv_b1, 0, False)
    lax.fori_loop(half, groups, group_step, 0)
    wait_b(recv_b1, 1)
    jones = jcur[...]
    pull = PENALTY * weight * (jones - target_of(recv_b1))
    mult = mult_ref[0] + pull
    jones = jones - STEP_SIZE * (data_slope() + mult + pull)
    mcur[...] = mult
    jcur[...] = jones
    fill_a(send_a2, mult, jones)
    send_a(send_a2, recv_a2, 2)

    acc[...] = jnp.zeros_like(acc)
    lax.fori_loop(0, half, group_step, 0)
    owner_turn(recv_a2, send_b2, recv_b2, 2, True)
    lax.fori_loop(half, groups, group_step, 0)
    wait_b(recv_b2, 3)
    jones = jcur[...]
    pull = PENALTY * weight * (jones - target_of(recv_b2))
    mult = mcur[...] + pull
    mout_ref[0] = mult
    jout_ref[0] = jones - STEP_SIZE * (data_slope() + mult + pull)
    shift = lax.rem(LANES - lax.rem(me * share, LANES), LANES)
    for p in range(3):
        part = pltpu.roll(recv_b2[pl.ds(4 + p, rows, stride=SUB), :], shift, 1)
        cout_ref[p * rows : (p + 1) * rows, :] = part[:, :share]

    for buf, phase in ((send_a1, 0), (send_a2, 2)):
        if all_own:
            wait_for(buf, rows - 1, send_sem.at[phase])
        else:
            when_owner(functools.partial(wait_for, buf, rows - 1, send_sem.at[phase]),
                       functools.partial(wait_for, buf, rows, send_sem.at[phase]))
    for buf, phase in ((send_b1, 1), (send_b2, 3)):
        when_owner(functools.partial(wait_for, buf, n - 1, send_sem.at[phase]))


def solution(mesh):
    n = mesh.shape["band"]

    def local(jones, visible, coherent, stations, weights, mult):
        rows, count = jones.shape[1:]
        base = visible.shape[2]
        chunks = count // LANES
        groups = base // GROUP
        assert n >= rows and chunks == 4 and LANES % (count // n) == 0
        f32, bf16 = jnp.float32, jnp.bfloat16
        vm = pltpu.VMEM
        flat = lambda slots: vm((slots * SUB, LANES), f32)
        return pl.pallas_call(
            functools.partial(kernel, n),
            out_shape=(
                jax.ShapeDtypeStruct(jones.shape, f32),
                jax.ShapeDtypeStruct(jones.shape, f32),
                jax.ShapeDtypeStruct((3 * rows, count // n), f32),
            ),
            in_specs=[pl.BlockSpec(memory_space=pltpu.HBM)] * 6,
            out_specs=[pl.BlockSpec(memory_space=vm)] * 3,
            scratch_shapes=[
                vm((rows, count), f32),
                vm((rows, count), f32),
                vm((groups, rows * SUB, LANES), f32),
                vm((groups, 8 * SUB, LANES), f32),
                vm((groups, 2 * SUB, LANES), jnp.int32),
                vm((groups, LANES, 2 * GROUP), bf16),
                flat(2 * rows),
                flat(rows),
                flat(2 * rows),
                vm((2 * chunks * rows, 2 * GROUP), bf16),
                vm((2 * chunks * rows, LANES), f32),
                flat(rows), flat(n), flat(n), flat(rows),
                flat(rows), flat(n), flat(n), flat(rows),
                flat(7), flat(3), flat(chunks),
                pltpu.SemaphoreType.DMA((4,)),
                pltpu.SemaphoreType.DMA((4,)),
                *[vm(v.shape, v.dtype) for v in (jones, visible, coherent, stations, weights, mult)],
                pltpu.SemaphoreType.DMA((6,)),
            ],
            compiler_params=pltpu.CompilerParams(
                collective_id=0, has_side_effects=True, vmem_limit_bytes=40 * 1024 * 1024),
        )(jones, visible, coherent, stations, weights, mult)

    return jax.shard_map(
        local,
        mesh=mesh,
        in_specs=(
            P("band", None, None), P("band", None, None), P("band", None, None),
            P(), P("band", None), P("band", None, None),
        ),
        out_specs=(P("band", None, None), P("band", None, None), P(None, "band")),
        check_vma=False,
    )
```

```python
import functools

import jax
import jax.numpy as jnp
from jax import lax
from jax.experimental import pallas as pl
from jax.experimental.pallas import tpu as pltpu
from jax.sharding import PartitionSpec as P

PENALTY = 1.0
STEP_SIZE = 0.05
MESH = pl.DeviceIdType.MESH
LANES = 128
SUB = 8
GROUP = LANES * SUB


def tile(index):
    return pl.ds(pl.multiple_of(index * SUB, SUB), SUB)


def cmul(a, b):
    return (a[0] * b[0] - a[1] * b[1], a[0] * b[1] + a[1] * b[0])


def cmul_conj(a, b):
    return (a[0] * b[0] + a[1] * b[1], a[1] * b[0] - a[0] * b[1])


def cadd(a, b):
    return (a[0] + b[0], a[1] + b[1])


def basis(f, n):
    x = -1.0 + f.astype(jnp.float32) * (2.0 / (n - 1))
    return x, 1.5 * x * x - 0.5


def kernel(
    n, jones_in, vis_in, coh_in, st_in, w_in, mult_in,
    jout_ref, mout_ref, cout_ref,
    jcur, mcur, cohv, visv, stv, oht, jgat, pbuf, dbuf, xbuf, acc,
    send_a1, recv_a1, send_b1, recv_b1, send_a2, recv_a2, send_b2, recv_b2,
    inv, coefs, ctile, send_sem, recv_sem,
    jones_ref, vis_ref, coh_ref, st_ref, w_ref, mult_ref, load_sem,
):
    loads = [
        pltpu.make_async_copy(src, dst, load_sem.at[i])
        for i, (src, dst) in enumerate((
            (jones_in, jones_ref), (mult_in, mult_ref), (w_in, w_ref),
            (coh_in, coh_ref), (vis_in, vis_ref), (st_in, st_ref)))
    ]
    for load in loads:
        load.start()
    me = lax.axis_index("band")
    rows, stations = jones_ref.shape[1:]
    baselines = vis_ref.shape[2]
    chunks = stations // LANES
    groups = baselines // GROUP
    dirs = rows // 8
    share = stations // n
    scale = stations / (2.0 * baselines)
    all_own = n == rows
    is_owner = me < rows

    def when_owner(fn, otherwise=None):
        if all_own:
            fn()
        else:
            pl.when(is_owner)(fn)
            if otherwise is not None:
                pl.when(jnp.logical_not(is_owner))(otherwise)

    barrier = pltpu.get_barrier_semaphore()

    def greet_all():
        def body(i, _):
            pl.semaphore_signal(barrier, inc=1, device_id=(lax.rem(me + i, n),), device_id_type=MESH)
            return 0
        lax.fori_loop(1, n, body, 0)

    def greet_owners():
        def body(i, _):
            pl.semaphore_signal(barrier, inc=1, device_id=(i,), device_id_type=MESH)
            return 0
        lax.fori_loop(0, rows, body, 0)

    when_owner(greet_all, greet_owners)

    for load in loads[:3]:
        load.wait()
    weight = w_ref[...]

    def fill_a(buf, m, j):
        comb = m + PENALTY * weight * j
        for h in range(chunks):
            cut = slice(h * LANES, (h + 1) * LANES)
            buf[pl.ds(h, rows, stride=SUB), :] = comb[:, cut]
            buf[pl.ds(chunks + h, rows, stride=SUB), :] = jnp.broadcast_to(weight[:, cut], (rows, LANES))

    def copy(src, s_idx, dst, d_idx, phase, dest):
        return pltpu.make_async_remote_copy(
            src_ref=src.at[tile(s_idx)], dst_ref=dst.at[tile(d_idx)],
            send_sem=send_sem.at[phase], recv_sem=recv_sem.at[phase],
            device_id=(dest,), device_id_type=MESH)

    def send_a(src, dst, phase):
        def body(i, _):
            c = lax.rem(me + i, rows)

            @pl.when(c != me)
            def _():
                copy(src, c, dst, me, phase, c).start()
            return 0

        if all_own:
            def body(i, _):
                c = lax.rem(me + i, rows)
                copy(src, c, dst, me, phase, c).start()
                return 0
            lax.fori_loop(1, rows, body, 0)
        else:
            lax.fori_loop(0, rows, body, 0)

        def own():
            dst[tile(me), :] = src[tile(me), :]
        when_owner(own)

    def send_b(src, dst, phase):
        def body(i, _):
            d = lax.rem(me + i, n)
            copy(src, d, dst, me, phase, d).start()
            return 0
        lax.fori_loop(1, n, body, 0)
        dst[tile(me), :] = src[tile(me), :]

    def wait_for(ref, slots, sem):
        part = ref.at[pl.ds(0, slots * SUB)]
        pltpu.make_async_copy(part, part, sem).wait()

    fill_a(send_a1, mult_ref[0], jones_ref[0])
    if all_own:
        pl.semaphore_wait(barrier, n - 1)
    else:
        when_owner(lambda: pl.semaphore_wait(barrier, n - 1), lambda: pl.semaphore_wait(barrier, rows))
    send_a(send_a1, recv_a1, 0)
    jcur[...] = jones_ref[0]
    for load in loads[3:]:
        load.wait()

    def prep(g, _):
        for s in range(SUB):
            cut = pl.ds(pl.multiple_of(g * GROUP + s * LANES, LANES), LANES)
            cohv[g, pl.ds(s, rows, stride=SUB), :] = coh_ref[0, :, cut].astype(jnp.float32)
            visv[g, pl.ds(s, 8, stride=SUB), :] = vis_ref[0, :, cut].astype(jnp.float32)
            for side in range(2):
                ids = st_ref[side : side + 1, cut]
                stv[g, side * SUB + s : side * SUB + s + 1, :] = ids
                low = jnp.broadcast_to(ids & (LANES - 1), (LANES, LANES))
                hot = low == lax.broadcasted_iota(jnp.int32, (LANES, LANES), 0)
                oht[g, :, side * GROUP + s * LANES : side * GROUP + (s + 1) * LANES] = jnp.where(hot, 1.0, 0.0).astype(jnp.bfloat16)
        return 0

    lax.fori_loop(0, groups, prep, 0)

    def group_step(g, _):
        ids = [stv[g, side * SUB : (side + 1) * SUB, :] for side in range(2)]
        low = [v & (LANES - 1) for v in ids]
        high = [v >> 7 for v in ids]
        pick = [[v == h for h in range(1, chunks)] for v in high]

        def station_value(side, c):
            out = None
            for h in range(chunks):
                row = jnp.broadcast_to(jcur[c : c + 1, h * LANES : (h + 1) * LANES], (SUB, LANES))
                got = jnp.take_along_axis(row, low[side], axis=1)
                out = got if h == 0 else jnp.where(pick[side][h - 1], got, out)
            return out

        def comp(ref, k, i, j):
            base = k * 8 + i * 2 + j
            return (ref(base), ref(base + 4))

        def tiles(ref, offset):
            return lambda c: ref[(offset + c) * SUB : (offset + c + 1) * SUB, :]

        coh = lambda c: cohv[g, c * SUB : (c + 1) * SUB, :]
        vis = lambda c: visv[g, c * SUB : (c + 1) * SUB, :]
        model = [[None, None], [None, None]]
        for k in range(dirs):
            for c in range(k * 8, k * 8 + 8):
                jgat[c * SUB : (c + 1) * SUB, :] = station_value(0, c)
                jgat[(rows + c) * SUB : (rows + c + 1) * SUB, :] = station_value(1, c)
            a = [[comp(tiles(jgat, 0), k, i, j) for j in range(2)] for i in range(2)]
            q = [[comp(tiles(jgat, rows), k, i, j) for j in range(2)] for i in range(2)]
            m = [[comp(coh, k, i, j) for j in range(2)] for i in range(2)]
            for i in range(2):
                inner = [cadd(cmul(a[i][0], m[0][j]), cmul(a[i][1], m[1][j])) for j in range(2)]
                for j in range(2):
                    base = k * 8 + i * 2 + j
                    pbuf[base * SUB : (base + 1) * SUB, :] = inner[j][0]
                    pbuf[(base + 4) * SUB : (base + 5) * SUB, :] = inner[j][1]
                    term = cadd(cmul_conj(inner[0], q[j][0]), cmul_conj(inner[1], q[j][1]))
                    model[i][j] = term if model[i][j] is None else cadd(model[i][j], term)
        resid = [[None, None], [None, None]]
        for i in range(2):
            for j in range(2):
                v = comp(vis, 0, i, j)
                resid[i][j] = tuple((-2.0 * scale) * (v[z] - model[i][j][z]) for z in range(2))
        for k in range(dirs):
            q = [[comp(tiles(jgat, rows), k, i, j) for j in range(2)] for i in range(2)]
            m = [[comp(coh, k, i, j) for j in range(2)] for i in range(2)]
            p = [[comp(tiles(pbuf, 0), k, i, j) for j in range(2)] for i in range(2)]
            for i in range(2):
                x = [cadd(cmul(resid[i][0], q[0][l]), cmul(resid[i][1], q[1][l])) for l in range(2)]
                for j in range(2):
                    ga = cadd(cmul_conj(x[0], m[j][0]), cmul_conj(x[1], m[j][1]))
                    gq = cadd(cmul_conj(p[0][j], resid[0][i]), cmul_conj(p[1][j], resid[1][i]))
                    base = k * 8 + i * 2 + j
                    for z in range(2):
                        c = base + 4 * z
                        dbuf[c * SUB : (c + 1) * SUB, :] = ga[z]
                        dbuf[(rows + c) * SUB : (rows + c + 1) * SUB, :] = gq[z]
        for side in range(2):
            for s in range(SUB):
                d = dbuf[pl.ds(side * rows * SUB + s, rows, stride=SUB), :]
                big = d.astype(jnp.bfloat16)
                small = (d - big.astype(jnp.float32)).astype(jnp.bfloat16)
                which = jnp.broadcast_to(high[side][s : s + 1, :], (rows, LANES))
                at = slice(side * GROUP + s * LANES, side * GROUP + (s + 1) * LANES)
                for h in range(chunks):
                    mask = jnp.where(which == h, 1.0, 0.0).astype(jnp.bfloat16)
                    xbuf[(2 * h) * rows : (2 * h + 1) * rows, at] = big * mask
                    xbuf[(2 * h + 1) * rows : (2 * h + 2) * rows, at] = small * mask
        acc[...] += lax.dot_general(
            xbuf[...], oht[g], (((1,), (1,)), ((), ())), preferred_element_type=jnp.float32)
        return 0

    def data_slope():
        parts = [
            acc[2 * h * rows : (2 * h + 1) * rows, :] + acc[(2 * h + 1) * rows : (2 * h + 2) * rows, :]
            for h in range(chunks)
        ]
        return jnp.concatenate(parts, axis=1)

    row_id = lax.broadcasted_iota(jnp.int32, (SUB, LANES), 0)

    def solve(recv, send, last):
        zero = jnp.zeros((SUB, LANES), jnp.float32)
        if not last:
            def add(f, sums):
                x, y = basis(f, n)
                t = recv[tile(f), :]
                tx, ty = t * x, t * y
                new = (t, tx, ty, tx * x, tx * y, ty * y)
                return tuple(o + v for o, v in zip(sums, new))

            sums = lax.fori_loop(0, n, add, (zero,) * 6, unroll=4)
            aa, ab, ac, bb, bc, cc = [PENALTY * pltpu.roll(v, chunks, 0) for v in sums]
            c_aa = bb * cc - bc * bc
            c_ab = ac * bc - ab * cc
            c_ac = ab * bc - ac * bb
            c_bb = aa * cc - ac * ac
            c_bc = ab * ac - aa * bc
            c_cc = aa * bb - ab * ab
            det = aa * c_aa + ab * c_ab + ac * c_ac
            cof = (c_aa, c_ab, c_ac, c_bb, c_bc, c_cc, 1.0 / det)
            for i, v in enumerate(cof):
                inv[i * SUB : (i + 1) * SUB, :] = v
            right = sums[:3]
        else:
            def add(f, sums):
                x, y = basis(f, n)
                t = recv[tile(f), :]
                return (sums[0] + t, sums[1] + t * x, sums[2] + t * y)

            right = lax.fori_loop(0, n, add, (zero,) * 3, unroll=4)
            cof = [inv[i * SUB : (i + 1) * SUB, :] for i in range(7)]
        c_aa, c_ab, c_ac, c_bb, c_bc, c_cc, inv_det = cof
        r0, r1, r2 = right
        k0 = (c_aa * r0 + c_ab * r1 + c_ac * r2) * inv_det
        k1 = (c_ab * r0 + c_bb * r1 + c_bc * r2) * inv_det
        k2 = (c_ac * r0 + c_bc * r1 + c_cc * r2) * inv_det
        if last:
            ctile[...] = jnp.zeros_like(ctile)
            for p, v in enumerate((k0, k1, k2)):
                coefs[p * SUB : (p + 1) * SUB, :] = v
            for h in range(chunks):
                for p in range(3):
                    ctile[h * SUB + 4 + p : h * SUB + 5 + p, :] = coefs[p * SUB + h : p * SUB + h + 1, :]

        def put(f, _):
            x, y = basis(f, n)
            t = k0 + x * k1 + y * k2
            if last:
                t = jnp.where(row_id < chunks, t, ctile[tile((f * share) // LANES), :])
            send[tile(f), :] = t
            return 0

        lax.fori_loop(0, n, put, 0, unroll=4)

    def owner_turn(recv_a, send_bb, recv_bb, phase, last):
        def go():
            wait_for(recv_a, n - 1, recv_sem.at[phase])
            solve(recv_a, send_bb, last)
            send_b(send_bb, recv_bb, phase + 1)
        when_owner(go)

    def wait_b(recv_bb, phase):
        if all_own:
            wait_for(recv_bb, rows - 1, recv_sem.at[phase])
        else:
            when_owner(lambda: wait_for(recv_bb, rows - 1, recv_sem.at[phase]),
                       lambda: wait_for(recv_bb, rows, recv_sem.at[phase]))

    def target_of(recv_bb):
        return jnp.concatenate([recv_bb[pl.ds(h, rows, stride=SUB), :] for h in range(chunks)], axis=1)

    half = groups // 2

    acc[...] = jnp.zeros_like(acc)
    lax.fori_loop(0, half, group_step, 0)
    owner_turn(recv_a1, send_b1, recv_b1, 0, False)
    lax.fori_loop(half, groups, group_step, 0)
    wait_b(recv_b1, 1)
    jones = jcur[...]
    pull = PENALTY * weight * (jones - target_of(recv_b1))
    mult = mult_ref[0] + pull
    jones = jones - STEP_SIZE * (data_slope() + mult + pull)
    mcur[...] = mult
    jcur[...] = jones
    fill_a(send_a2, mult, jones)
    send_a(send_a2, recv_a2, 2)

    acc[...] = jnp.zeros_like(acc)
    lax.fori_loop(0, half, group_step, 0)
    owner_turn(recv_a2, send_b2, recv_b2, 2, True)
    lax.fori_loop(half, groups, group_step, 0)
    wait_b(recv_b2, 3)
    jones = jcur[...]
    pull = PENALTY * weight * (jones - target_of(recv_b2))
    mult = mcur[...] + pull
    mout_ref[0] = mult
    jout_ref[0] = jones - STEP_SIZE * (data_slope() + mult + pull)
    shift = lax.rem(LANES - lax.rem(me * share, LANES), LANES)
    for p in range(3):
        part = pltpu.roll(recv_b2[pl.ds(4 + p, rows, stride=SUB), :], shift, 1)
        cout_ref[p * rows : (p + 1) * rows, :] = part[:, :share]

    for buf, phase in ((send_a1, 0), (send_a2, 2)):
        if all_own:
            wait_for(buf, rows - 1, send_sem.at[phase])
        else:
            when_owner(functools.partial(wait_for, buf, rows - 1, send_sem.at[phase]),
                       functools.partial(wait_for, buf, rows, send_sem.at[phase]))
    for buf, phase in ((send_b1, 1), (send_b2, 3)):
        when_owner(functools.partial(wait_for, buf, n - 1, send_sem.at[phase]))


def solution(mesh):
    n = mesh.shape["band"]

    def local(jones, visible, coherent, stations, weights, mult):
        rows, count = jones.shape[1:]
        base = visible.shape[2]
        chunks = count // LANES
        groups = base // GROUP
        assert n >= rows and chunks == 4 and LANES % (count // n) == 0
        f32, bf16 = jnp.float32, jnp.bfloat16
        vm = pltpu.VMEM
        flat = lambda slots: vm((slots * SUB, LANES), f32)
        return pl.pallas_call(
            functools.partial(kernel, n),
            out_shape=(
                jax.ShapeDtypeStruct(jones.shape, f32),
                jax.ShapeDtypeStruct(jones.shape, f32),
                jax.ShapeDtypeStruct((3 * rows, count // n), f32),
            ),
            in_specs=[pl.BlockSpec(memory_space=pltpu.HBM)] * 6,
            out_specs=[pl.BlockSpec(memory_space=vm)] * 3,
            scratch_shapes=[
                vm((rows, count), f32),
                vm((rows, count), f32),
                vm((groups, rows * SUB, LANES), f32),
                vm((groups, 8 * SUB, LANES), f32),
                vm((groups, 2 * SUB, LANES), jnp.int32),
                vm((groups, LANES, 2 * GROUP), bf16),
                flat(2 * rows),
                flat(rows),
                flat(2 * rows),
                vm((2 * chunks * rows, 2 * GROUP), bf16),
                vm((2 * chunks * rows, LANES), f32),
                flat(rows), flat(n), flat(n), flat(rows),
                flat(rows), flat(n), flat(n), flat(rows),
                flat(7), flat(3), flat(chunks),
                pltpu.SemaphoreType.DMA((4,)),
                pltpu.SemaphoreType.DMA((4,)),
                *[vm(v.shape, v.dtype) for v in (jones, visible, coherent, stations, weights, mult)],
                pltpu.SemaphoreType.DMA((6,)),
            ],
            compiler_params=pltpu.CompilerParams(
                collective_id=0, has_side_effects=True, vmem_limit_bytes=64 * 1024 * 1024),
        )(jones, visible, coherent, stations, weights, mult)

    return jax.shard_map(
        local,
        mesh=mesh,
        in_specs=(
            P("band", None, None), P("band", None, None), P("band", None, None),
            P(), P("band", None), P("band", None, None),
        ),
        out_specs=(P("band", None, None), P("band", None, None), P(None, "band")),
        check_vma=False,
    )
```
